32 devices in a mesh: section: 4 (over x, core), dp: 8 (over z, y).
Axes of the slice: x: 2, y: 2, z: 4, core: 2. Of those that a mesh axis runs over, the one named last changes fastest.
Arguments:
- obs_features: bfloat16 [4, 256, 1024], P(None, 'dp'), may hold values from -1.1953125 to 1.1953125
- w_input: bfloat16 [4, 1024, 4096], P('section'), may hold values from -1 to 1
- w_recurrent: bfloat16 [4, 1024, 4096], P('section', None, 'dp'), may hold values from -0.1875 to 0.1875
- bias: float32 [4, 4096], P('section'), may hold values from -3 to 3
- stored_states: bfloat16 [4, 4, 256, 2048], P('section', None, 'dp'), may hold values from -3 to 3
- state_owner: int32 [256], P('dp'), may hold values from 0 to 3
- burn_steps: int32 [256], P('dp'), may hold values from 1 to 2
- valid_steps: int32 [256], P('dp'), may hold values from 3 to 4
- cotangent: bfloat16 [4, 256, 1024], P(None, 'dp'), may hold values from -3 to 3
Outputs:
- hidden_all: bfloat16 [4, 4, 256, 1024], P('section', None, 'dp')
- grad_recurrent: float32 [4, 1024, 4096], P('section', None, 'dp')
- grad_bias: float32 [4, 4096], P('section', 'dp')
The draws below stay inside these ranges and needn't reach their ends.
All inputs are finite; a program needn't handle non-finite values.
Results may differ from the reference program's by a relative error of at most 0.017.
Values may be sent and summed in bfloat16 or wider, within the bound.
No kernel may reach another device: no remote copies, remote signals or barrier semaphores. Data moves between devices by JAX's collectives and lax.ppermute only.
A program may use at most 128 MiB of HBM per device.

```python
import jax
import jax.numpy as jnp
from jax import lax

D = 1024
GATES = 4096
LAYERS = 4
SEQS = 256
STEPS = 4
BURN = 2
N_SECTION = 4


def set_ends(array, own_key, low, high):
    spot = [jax.random.randint(jax.random.fold_in(own_key, axis), (), 0, length) for axis, length in enumerate(array.shape)]
    main_axis = array.shape.index(max(array.shape))
    next_to = spot[:main_axis] + [(spot[main_axis] + 1) % array.shape[main_axis]] + spot[main_axis + 1:]
    return array.at[tuple(spot)].set(low).at[tuple(next_to)].set(high)


def shard_levels(own_key, dims, pieces, least, high):
    def one(dim, parts):
        heights = jax.random.uniform(jax.random.fold_in(jax.random.fold_in(own_key, 6), dim), (parts,), jnp.float32, least / len(pieces), high / len(pieces))
        return jnp.repeat(jnp.exp(heights), dims[dim] // parts).reshape((-1,) + (1,) * (len(dims) - dim - 1))

    loudness = one(*pieces[0])
    for cut in pieces[1:]:
        loudness = loudness * one(*cut)
    return loudness


def bell_draw(rng, shape, deviation, reach, pieces=(), kind=jnp.bfloat16):
    array = jax.random.normal(rng, shape, jnp.float32) * deviation
    if len(pieces) > 0:
        array = shard_levels(rng, shape, pieces, -0.22, 0.18) * array
    return jnp.clip(array, min=-reach, max=reach).astype(kind)


def setup_inputs(seed: int = 0) -> dict:
    arg_keys = jax.random.split(jax.random.key(seed), 10)
    return {
        "obs_features": bell_draw(arg_keys[0], (STEPS, SEQS, D), 0.2, 1.1953125, ((1, 8),)),
        "w_input": bell_draw(arg_keys[1], (LAYERS, D, GATES), (D // 25) ** -0.5, 1.0, ((0, 4),)),
        "w_recurrent": bell_draw(arg_keys[2], (LAYERS, D, GATES), D ** -0.5, 0.1875, ((0, 4), (2, 8))),
        "bias": bell_draw(arg_keys[3], (LAYERS, GATES), 0.5, 3.0, ((0, 4),), jnp.float32),
        "stored_states": bell_draw(arg_keys[4], (N_SECTION, LAYERS, SEQS, 2 * D), 0.5, 3.0, ((0, 4), (2, 8))),
        "state_owner": set_ends(jax.random.randint(arg_keys[5], (SEQS,), 0, N_SECTION), jax.random.fold_in(arg_keys[5], 1), 0, N_SECTION - 1).astype(jnp.int32),
        "burn_steps": set_ends(jax.random.randint(arg_keys[6], (SEQS,), BURN // 2, BURN + 1), jax.random.fold_in(arg_keys[6], 1), BURN // 2, BURN).astype(jnp.int32),
        "valid_steps": set_ends(jax.random.randint(arg_keys[7], (SEQS,), STEPS - (STEPS - BURN) // 2, STEPS + 1), jax.random.fold_in(arg_keys[7], 1), STEPS - (STEPS - BURN) // 2, STEPS).astype(jnp.int32),
        "cotangent": bell_draw(arg_keys[8], (STEPS, SEQS, D), 0.5, 3.0, ((1, 8),)),
    }


def lstm_cell(preact, cell_prev):
    breadth = cell_prev.shape[-1]
    in_gate = jax.nn.sigmoid(preact[:, :breadth])
    forget = jax.nn.sigmoid(preact[:, breadth:2 * breadth])
    candidate = jnp.tanh(preact[:, 2 * breadth:3 * breadth])
    out_gate = jax.nn.sigmoid(preact[:, 3 * breadth:])
    cell_new = forget * cell_prev + in_gate * candidate
    hidden_new = (out_gate * jnp.tanh(cell_new)).astype(jnp.bfloat16)
    gate_vals = jnp.concatenate([in_gate, forget, candidate, out_gate], axis=-1)
    return hidden_new, cell_new, gate_vals


def forward_span(inputs, w_in, w_rec, bias_row, hidden_start, cell_start):
    step_count, seq_rows, breadth = inputs.shape
    projected = jnp.dot(inputs.reshape(step_count * seq_rows, breadth), w_in, preferred_element_type=jnp.float32)
    projected = projected.reshape(step_count, seq_rows, -1) + bias_row

    def advance(carried, proj_row):
        hidden_prev, cell_prev = carried
        preact = proj_row + jnp.dot(hidden_prev, w_rec, preferred_element_type=jnp.float32)
        hidden_new, cell_new, gate_vals = lstm_cell(preact, cell_prev)
        return (hidden_new, cell_new), (hidden_new, cell_new, gate_vals)

    (hidden_end, cell_end), (hidden_seq, cell_seq, gate_seq) = lax.scan(advance, (hidden_start, cell_start), projected)
    return hidden_seq, cell_seq, gate_seq, hidden_end, cell_end


def times_transposed(operand, matrix):
    return lax.dot_general(operand, matrix, (((1,), (1,)), ((), ())), preferred_element_type=jnp.float32)


def backward_span(above_grads, cell_now, cell_old, gate_seq, live_mask, w_rec, grad_h, grad_c):
    def retreat(carried, inputs):
        grad_hidden, grad_cell = carried
        grad_out, cell_cur, cell_before, gate_vals, alive_row = inputs
        breadth = cell_cur.shape[-1]
        in_gate = gate_vals[:, :breadth]
        forget = gate_vals[:, breadth:2 * breadth]
        candidate = gate_vals[:, 2 * breadth:3 * breadth]
        out_gate = gate_vals[:, 3 * breadth:]
        total_h = grad_out.astype(jnp.float32) + grad_hidden
        squashed = jnp.tanh(cell_cur)
        total_c = grad_cell + total_h * out_gate * (1.0 - squashed * squashed)
        grad_pre = jnp.concatenate([
            total_c * candidate * in_gate * (1.0 - in_gate),
            total_c * cell_before * forget * (1.0 - forget),
            total_c * in_gate * (1.0 - candidate * candidate),
            total_h * squashed * out_gate * (1.0 - out_gate)], axis=-1) * alive_row[:, None]
        gate_grads = grad_pre.astype(jnp.bfloat16)
        return (times_transposed(gate_grads, w_rec), total_c * forget * alive_row[:, None]), gate_grads

    (grad_h_end, grad_c_end), gate_grads = lax.scan(
        retreat, (grad_h, grad_c), (above_grads, cell_now, cell_old, gate_seq, live_mask), reverse=True)
    return gate_grads, grad_h_end, grad_c_end


def reference(obs_features, w_input, w_recurrent, bias, stored_states, state_owner, burn_steps, valid_steps, cotangent):
    breadth = w_input.shape[1]
    seq_rows = obs_features.shape[1]
    owners = jnp.arange(N_SECTION, dtype=jnp.int32)
    picked = (state_owner[None, :] == owners[:, None])[:, :, None]
    positions = jnp.arange(STEPS, dtype=jnp.int32)[:, None]
    live_mask = ((positions >= burn_steps[None, :]) & (positions < valid_steps[None, :])).astype(jnp.float32)
    layer_input = obs_features
    stored_acts = []
    hidden_list = []
    for layer_index in range(LAYERS):
        delivered = jnp.sum(jnp.where(picked, stored_states[:, layer_index].astype(jnp.float32), jnp.float32(0.0)), axis=0)
        hidden_start = delivered[:, :breadth].astype(jnp.bfloat16)
        cell_start = delivered[:, breadth:]
        hidden_seq, cell_seq, gate_seq, hidden_end, cell_end = forward_span(
            layer_input, w_input[layer_index], w_recurrent[layer_index], bias[layer_index], hidden_start, cell_start)
        hidden_full = jnp.concatenate([hidden_start[None], hidden_seq], axis=0)
        cell_full = jnp.concatenate([cell_start[None], cell_seq], axis=0)
        stored_acts.append((hidden_full, cell_full, gate_seq))
        hidden_list.append(hidden_seq)
        layer_input = hidden_seq
    above_grads = cotangent
    weight_list = []
    bias_list = []
    zero_state = jnp.zeros((seq_rows, breadth), jnp.float32)
    for layer_index in range(LAYERS - 1, -1, -1):
        hidden_full, cell_full, gate_seq = stored_acts[layer_index]
        gate_grads, grad_h_end, grad_c_end = backward_span(
            above_grads, cell_full[1:], cell_full[:-1], gate_seq, live_mask, w_recurrent[layer_index], zero_state, zero_state)
        gate_rows = gate_grads.reshape(STEPS * seq_rows, -1)
        prev_rows = hidden_full[:-1].reshape(STEPS * seq_rows, breadth)
        weight_list.append(jnp.dot(prev_rows.T, gate_rows, preferred_element_type=jnp.float32))
        bias_list.append(jnp.sum(gate_rows.astype(jnp.float32), axis=0))
        above_grads = times_transposed(gate_rows, w_input[layer_index]).reshape(STEPS, seq_rows, breadth).astype(jnp.bfloat16)
    weight_list = weight_list[::-1]
    bias_list = bias_list[::-1]
    return jnp.stack(hidden_list), jnp.stack(weight_list), jnp.stack(bias_list)
```

```python
from functools import partial

import jax
import jax.numpy as jnp
from jax import lax
from jax.experimental import pallas as pl
from jax.experimental.pallas import tpu as pltpu
from jax.sharding import PartitionSpec as P

AXES = ("section", "dp")
BF = jnp.bfloat16
F32 = jnp.float32
VMEM_SPEC = pl.BlockSpec(memory_space=pltpu.VMEM)
SMEM_SPEC = pl.BlockSpec(memory_space=pltpu.SMEM)
ANY_SPEC = pl.BlockSpec(memory_space=pl.ANY)
LANES = 128


class Roles:
    def __init__(self, sections, groups):
        self.sections, self.groups, self.half = sections, groups, groups // 2

    def home(self, layer, block):
        return layer * self.groups + block

    def device(self, layer, block):
        pair, high = layer // 2, (layer % 2) ^ (layer // 2 % 2)
        core, low = block // self.half, block % self.half
        return (2 * pair + core) * self.groups + high * self.half + low

    def each(self):
        return [(a, b) for a in range(self.sections) for b in range(self.groups)]

    def to_role(self):
        return [(self.home(a, b), self.device(a, b)) for a, b in self.each()]

    def to_home(self):
        return [(self.device(a, b), self.home(a, b)) for a, b in self.each()]

    def hop(self, by):
        return [
            (self.device(a, b), self.device(a + by, b))
            for a, b in self.each()
            if 0 <= a + by < self.sections
        ]

    def scatter(self, mix):
        return [(self.device(a, b), self.home(a, b ^ mix)) for a, b in self.each()]

    def section_shift(self, by):
        return [(self.home(a, b), self.home((a + by) % self.sections, b)) for a, b in self.each()]

    def mix(self, bits):
        return [(self.home(a, b), self.home(a, b ^ bits)) for a, b in self.each()]

    def layer_of(self, section, group):
        return 2 * (section // 2) + ((group // self.half) ^ (section // 2 % 2))

    def block_of(self, section, group):
        return group % self.half + self.half * (section % 2)

    def from_partner(self):
        pairs = []
        for s, g in self.each():
            if self.layer_of(s, g) != s:
                pairs.append((self.home(s ^ 1, g), self.home(s, g)))
        return pairs


def move(array, pairs):
    return lax.ppermute(array, AXES, pairs)


def rec_body(h_ref, w_ref, bias_ref, z_ref):
    h = h_ref[...]
    count, _, width = w_ref.shape
    for i in range(count):
        cols = slice(i * width, (i + 1) * width)
        z_ref[:, cols] = jnp.dot(h, w_ref[i], preferred_element_type=F32) + bias_ref[:, cols]


def rec_part(h, w_rec, bias_row):
    rows, gates = h.shape[0], bias_row.shape[1]
    return pl.pallas_call(
        rec_body,
        out_shape=jax.ShapeDtypeStruct((rows, gates), F32),
        in_specs=[VMEM_SPEC] * 3,
        out_specs=VMEM_SPEC,
        name="rec_part",
        compiler_params=pltpu.CompilerParams(vmem_limit_bytes=24 * 2**20),
        cost_estimate=pl.CostEstimate(
            flops=2 * rows * w_rec.size, bytes_accessed=2 * w_rec.size, transcendentals=0
        ),
    )(h, w_rec, bias_row)


def cell_body(flags, obs_ref, inc_ref, z_ref, h_ref, c_ref, w_ref, h_out, c_out, gates_out):
    breadth = c_ref.shape[1]
    step = min(256, breadth)
    bottom, active = flags[0] > 0, flags[1] > 0
    x = jnp.where(bottom, obs_ref[...], inc_ref[...])
    for u in range(0, breadth, step):
        own = slice(u, u + step)
        pre = []
        for q in range(4):
            cols = slice(q * breadth + u, q * breadth + u + step)
            pre.append(z_ref[:, cols] + jnp.dot(x, w_ref[:, cols], preferred_element_type=F32))
        i = jax.nn.sigmoid(pre[0])
        f = jax.nn.sigmoid(pre[1])
        g = jnp.tanh(pre[2])
        o = jax.nn.sigmoid(pre[3])
        c_old = c_ref[:, own]
        c_new = f * c_old + i * g
        h_new = (o * jnp.tanh(c_new)).astype(BF)
        h_out[:, own] = jnp.where(active, h_new, h_ref[:, own])
        c_out[:, own] = jnp.where(active, c_new, c_old)
        for q, value in enumerate((i, f, g, o)):
            gates_out[:, q * breadth + u : q * breadth + u + step] = value


def cell_part(flags, obs, inc, z, h, c, w_in):
    rows, breadth = c.shape
    return pl.pallas_call(
        cell_body,
        out_shape=(
            jax.ShapeDtypeStruct((rows, breadth), BF),
            jax.ShapeDtypeStruct((rows, breadth), F32),
            jax.ShapeDtypeStruct((rows, 4 * breadth), F32),
        ),
        in_specs=[SMEM_SPEC] + [VMEM_SPEC] * 6,
        out_specs=(VMEM_SPEC,) * 3,
        name="cell_part",
        compiler_params=pltpu.CompilerParams(vmem_limit_bytes=24 * 2**20),
        cost_estimate=pl.CostEstimate(
            flops=2 * rows * w_in.size, bytes_accessed=2 * w_in.size, transcendentals=0
        ),
    )(flags, obs, inc, z, h, c, w_in)


def nt_dot(a, b):
    return lax.dot_general(a, b, (((1,), (1,)), ((), ())), preferred_element_type=F32)


def grad_body(
    flags, cot_ref, inc_ref, a_ref, k_ref, gates_ref, c_ref, old_ref, live_ref, w_ref, g_out, k_out, e_out
):
    breadth = c_ref.shape[1]
    step = min(256, breadth)
    top = flags[0] > 0
    live = live_ref[:, 0:1].astype(F32) * jnp.where(flags[1] > 0, 1.0, 0.0)
    total = None
    for u in range(0, breadth, step):
        own = slice(u, u + step)
        cols = [slice(q * breadth + u, q * breadth + u + step) for q in range(4)]
        i, f, g, o = [gates_ref[:, col] for col in cols]
        above = jnp.where(top, cot_ref[:, own], inc_ref[:, own]).astype(F32)
        dh = above + a_ref[:, own]
        squashed = jnp.tanh(c_ref[:, own])
        dc = k_ref[:, own] + dh * o * (1.0 - squashed * squashed)
        parts = (
            dc * g * i * (1.0 - i),
            dc * old_ref[:, own] * f * (1.0 - f),
            dc * i * (1.0 - g * g),
            dh * squashed * o * (1.0 - o),
        )
        k_out[:, own] = dc * f * live
        for col, part in zip(cols, parts):
            rounded = (part * live).astype(BF)
            g_out[:, col] = rounded
            product = nt_dot(rounded, w_ref[:, col])
            total = product if total is None else total + product
    e_out[...] = total.astype(BF)


def grad_part(flags, cot, inc, a, k, gates, c, c_old, live, w_in):
    rows, breadth = c.shape
    return pl.pallas_call(
        grad_body,
        out_shape=(
            jax.ShapeDtypeStruct((rows, 4 * breadth), BF),
            jax.ShapeDtypeStruct((rows, breadth), F32),
            jax.ShapeDtypeStruct((rows, breadth), BF),
        ),
        in_specs=[SMEM_SPEC] + [VMEM_SPEC] * 9,
        out_specs=(VMEM_SPEC,) * 3,
        name="grad_part",
        compiler_params=pltpu.CompilerParams(vmem_limit_bytes=24 * 2**20),
        cost_estimate=pl.CostEstimate(
            flops=2 * rows * w_in.size, bytes_accessed=2 * w_in.size, transcendentals=0
        ),
    )(flags, cot, inc, a, k, gates, c, c_old, live, w_in)


def back_body(g_ref, w_ref, a_ref):
    count, _, width = w_ref.shape
    total = None
    for i in range(count):
        product = nt_dot(g_ref[:, i * width : (i + 1) * width], w_ref[i])
        total = product if total is None else total + product
    a_ref[...] = total


def back_part(g, w_rec):
    rows, breadth = g.shape[0], w_rec.shape[1]
    return pl.pallas_call(
        back_body,
        out_shape=jax.ShapeDtypeStruct((rows, breadth), F32),
        in_specs=[VMEM_SPEC] * 2,
        out_specs=VMEM_SPEC,
        name="back_part",
        compiler_params=pltpu.CompilerParams(vmem_limit_bytes=24 * 2**20),
        cost_estimate=pl.CostEstimate(
            flops=2 * rows * w_rec.size, bytes_accessed=2 * w_rec.size, transcendentals=0
        ),
    )(g, w_rec)


def collect_body(ids, *refs):
    count = (len(refs) - 2) // 2
    own, other, out, sems = refs[:count], refs[count : 2 * count], refs[-2], refs[-1]

    def copies(sources):
        return [
            pltpu.make_async_copy(ref, out.at[ids[i]], sems.at[i]) for i, ref in enumerate(sources)
        ]

    @pl.when(ids[count] > 0)
    def _():
        for copy in copies(own):
            copy.start()

    @pl.when(ids[count] <= 0)
    def _():
        for copy in copies(other):
            copy.start()

    for copy in copies(own):
        copy.wait()


def collect(ids, own, other):
    count = len(own)
    return pl.pallas_call(
        collect_body,
        out_shape=jax.ShapeDtypeStruct((count, *own[0].shape), own[0].dtype),
        in_specs=[SMEM_SPEC] + [ANY_SPEC] * (2 * count),
        out_specs=VMEM_SPEC,
        scratch_shapes=[pltpu.SemaphoreType.DMA((count,))],
        name="collect",
        compiler_params=pltpu.CompilerParams(vmem_limit_bytes=24 * 2**20),
    )(ids, *own, *other)


def gather_columns(roles, block, section, group, at_home):
    partner = roles.from_partner()
    if roles.groups != 8:
        whole = lax.all_gather(block, "dp", axis=1, tiled=True)
        return jnp.where(at_home, whole, move(whole, partner))[None]
    far = [(a, y) for a in range(roles.sections) for y in range(2)]

    def spot(layer, m, y):
        high = (layer % 2) ^ (layer // 2 % 2)
        return roles.home(layer, 2 * (3 - m if high else m) + y)

    high = group // 4
    place = jnp.where(high > 0, 3 - group // 2, group // 2)
    step1 = [(spot(a, m, y), spot(a, m - 1, y)) for a, y in far for m in (1, 2, 3)]
    step2 = [(spot(a, m, y), spot(a, m - 1, y)) for a, y in far for m in (1, 2)]
    step3 = [(spot(a, 1, y), spot(a, 0, y)) for a, y in far]
    step3 += [(spot(a, 0, y), spot(a, 1, y)) for a, y in far]
    across = [(spot(a, m, y), spot(a, m, 1 - y)) for a, y in far for m in (0, 1)]
    slots = [block]
    slots.append(move(block, step1))
    slots.append(move(slots[1], step2))
    slots.append(move(jnp.where(place == 0, block, slots[2]), step3))
    slots += [move(slot, across) for slot in slots]
    others = [move(slot, partner) for slot in slots]
    mirrored = [(place + i) % 4 for i in range(4)]
    lines = [jnp.where(high > 0, 3 - m, m) for m in mirrored]
    side = group % 2
    ids = [2 * q + side for q in lines] + [2 * q + 1 - side for q in lines]
    ids.append(at_home.astype(jnp.int32))
    return collect(jnp.stack(ids), slots, others)


def gather_rows(roles, rows):
    if roles.groups != 8:
        return lax.all_gather(rows, "dp", axis=0, tiled=False)
    line = [rows] + [move(rows, roles.mix(2 * k)) for k in (1, 2, 3)]
    line = jnp.stack(line)
    beside = move(line, roles.mix(1))
    return jnp.stack([line, beside], axis=1).reshape(8, *rows.shape)


def scatter_columns(roles, grads, block_index):
    groups = roles.groups
    width = grads.shape[-1] // groups
    if groups != 8:
        moved = move(grads, roles.to_home())
        moved = lax.all_to_all(moved, "dp", split_axis=1, concat_axis=0, tiled=True)
        return moved.reshape(groups, -1, width)
    pieces = []
    for k in range(groups):
        piece = lax.dynamic_slice_in_dim(grads, (block_index ^ k) * width, width, 1)
        pieces.append(move(piece, roles.scatter(k)))
    return jnp.stack(pieces)


def on_device(
    obs_features,
    w_input,
    w_recurrent,
    bias,
    stored_states,
    state_owner,
    burn_steps,
    valid_steps,
    cotangent,
):
    sections, groups = lax.axis_size("section"), lax.axis_size("dp")
    section, group = lax.axis_index("section"), lax.axis_index("dp")
    roles = Roles(sections, groups)
    steps, rows, breadth = obs_features.shape
    pair, core = section // 2, section % 2
    layer = 2 * pair + ((group // roles.half) ^ (pair % 2))
    block_index = group % roles.half + roles.half * core
    at_home = layer == section
    partner = roles.from_partner()

    owned = (state_owner == section)[None, :, None]
    table = jnp.where(owned, stored_states[0], jnp.zeros((), BF))
    start = lax.dynamic_index_in_dim(table, section, 0, keepdims=False)
    for k in range(1, sections):
        part = lax.dynamic_index_in_dim(table, (section + k) % sections, 0, keepdims=False)
        start = start + move(part, roles.section_shift(k))
    positions = jnp.arange(steps, dtype=jnp.int32)[:, None]
    live = ((positions >= burn_steps[None, :]) & (positions < valid_steps[None, :])).astype(BF)
    payload = jnp.concatenate(
        [
            jnp.where(section == sections - 1, cotangent, obs_features),
            jnp.broadcast_to(live[:, :, None], (steps, rows, LANES)),
        ],
        axis=-1,
    )
    payload = move(payload, roles.to_role())
    role_start = move(start, roles.to_role())
    edge, live = payload[..., :breadth], payload[..., breadth:]
    h = role_start[:, :breadth]
    c = role_start[:, breadth:].astype(F32)

    w_rec = gather_columns(roles, w_recurrent[0], section, group, at_home)
    w_in = jnp.where(at_home, w_input[0], move(w_input[0], partner))
    bias_row = jnp.where(at_home, bias, move(bias, partner))

    ticks = steps + sections - 1
    hs, cs, gate_list = [h], [c], []
    incoming = jnp.zeros((rows, breadth), BF)
    for tick in range(ticks):
        z = rec_part(h, w_rec, bias_row)
        t = tick - layer
        flags = jnp.stack([layer == 0, (t >= 0) & (t < steps)]).astype(jnp.int32)
        h, c, gates = cell_part(flags, edge[min(tick, steps - 1)], incoming, z, h, c, w_in)
        hs.append(h)
        cs.append(c)
        gate_list.append(gates)
        if tick + 1 < ticks:
            incoming = move(h, roles.hop(1))

    hidden = lax.dynamic_slice_in_dim(jnp.stack(hs[1:]), layer, steps, 0)
    hidden = move(hidden, roles.to_home())
    before = jnp.concatenate([start[None, :, :breadth], hidden[:-1]], axis=0)
    before = gather_rows(roles, before.reshape(steps * rows, breadth))

    grad_list = [None] * ticks
    a = jnp.zeros((rows, breadth), F32)
    k = jnp.zeros((rows, breadth), F32)
    incoming = jnp.zeros((rows, breadth), BF)
    for tick in range(ticks - 1, -1, -1):
        t = tick - layer
        flags = jnp.stack([layer == sections - 1, (t >= 0) & (t < steps)]).astype(jnp.int32)
        alive = lax.dynamic_index_in_dim(live, jnp.clip(t, 0, steps - 1), 0, keepdims=False)
        grads, k, lower = grad_part(
            flags,
            edge[max(tick - sections + 1, 0)],
            incoming,
            a,
            k,
            gate_list[tick],
            cs[tick + 1],
            cs[tick],
            alive,
            w_in,
        )
        grad_list[tick] = grads
        if tick > 0:
            incoming = move(lower, roles.hop(-1))
            a = back_part(grads, w_rec)

    grads = lax.dynamic_slice_in_dim(jnp.stack(grad_list), layer, steps, 0)
    columns = scatter_columns(roles, grads.reshape(steps * rows, -1), block_index)
    columns = columns.reshape(-1, columns.shape[-1])
    weight_grad = lax.dot_general(
        before.reshape(-1, breadth),
        columns,
        (((0,), (0,)), ((), ())),
        preferred_element_type=F32,
    )
    bias_grad = jnp.sum(columns, axis=0, dtype=F32)
    return (hidden[None], weight_grad[None], bias_grad[None])


def solution(mesh):
    in_specs = (
        P(None, "dp", None),
        P("section", None, None),
        P("section", None, "dp"),
        P("section", None),
        P("section", None, "dp", None),
        P("dp"),
        P("dp"),
        P("dp"),
        P(None, "dp", None),
    )
    out_specs = (P("section", None, "dp", None), P("section", None, "dp"), P("section", "dp"))
    return jax.shard_map(
        on_device, mesh=mesh, in_specs=in_specs, out_specs=out_specs, check_vma=False
    )
```

```python
from functools import partial

import jax
import jax.numpy as jnp
import numpy as np
from jax import lax
from jax.experimental import pallas as pl
from jax.experimental.pallas import tpu as pltpu
from jax.sharding import PartitionSpec as P


AXES = ("section", "dp")
BF = jnp.bfloat16
F32 = jnp.float32
VMEM_SPEC = pl.BlockSpec(memory_space=pltpu.VMEM)
SMEM_SPEC = pl.BlockSpec(memory_space=pltpu.SMEM)
ANY_SPEC = pl.BlockSpec(memory_space=pl.ANY)
LANES = 128
LIMIT = 12 * 2**20
OUTER_LIMIT = 40 * 2**20


class Roles:
    def __init__(self, sections, groups):
        self.sections, self.groups, self.half = sections, groups, groups // 2

    def home(self, layer, block):
        return layer * self.groups + block

    def device(self, layer, block):
        pair, high = layer // 2, (layer % 2) ^ (layer // 2 % 2)
        core, low = block // self.half, block % self.half
        return (2 * pair + core) * self.groups + high * self.half + low

    def each(self):
        return [(a, b) for a in range(self.sections) for b in range(self.groups)]

    def to_role(self):
        return [(self.home(a, b), self.device(a, b)) for a, b in self.each()]

    def to_home(self):
        return [(self.device(a, b), self.home(a, b)) for a, b in self.each()]

    def hop(self, by):
        return [
            (self.device(a, b), self.device(a + by, b))
            for a, b in self.each()
            if 0 <= a + by < self.sections
        ]

    def scatter(self, mix):
        return [(self.device(a, b), self.home(a, b ^ mix)) for a, b in self.each()]

    def section_shift(self, by):
        return [(self.home(a, b), self.home((a + by) % self.sections, b)) for a, b in self.each()]

    def mix(self, bits):
        return [(self.home(a, b), self.home(a, b ^ bits)) for a, b in self.each()]

    def place(self, layer, block):
        high = (layer % 2) ^ (layer // 2 % 2)
        return 3 - block // 2 if high else block // 2

    def table(self, steps):
        ticks = steps + self.sections - 1
        found = {}
        for layer, block in self.each():
            at = self.device(layer, block)
            section, group = at // self.groups, at % self.groups
            t = np.arange(ticks) - layer
            row = {
                "at_home": [layer == section],
                "bottom": [layer == 0],
                "top": [layer == self.sections - 1],
                "layer": [layer],
                "section": [section],
                "last": [section == self.sections - 1],
                "shift": [(section + k) % self.sections for k in range(self.sections)],
                "active": (t >= 0) & (t < steps),
                "step": np.clip(t, 0, steps - 1),
                "column": [block ^ k for k in range(self.groups)],
            }
            if self.groups == 8:
                high = group // 4
                m = 3 - group // 2 if high else group // 2
                row["nearest"] = [m == 0]
                lines = [(m + j) % 4 for j in range(4)]
                lines = [3 - line if high else line for line in lines]
                side = group % 2
                row["slots"] = [2 * q + side for q in lines] + [2 * q + 1 - side for q in lines]
            found[at] = row
        places, at = {}, 0
        for key, value in found[0].items():
            places[key] = at
            at += len(value)
        rows = [np.concatenate([np.asarray(v) for v in found[d].values()]) for d in sorted(found)]
        return np.stack(rows).astype(np.int32), places

    def partner(self):
        return [(self.home(s, g), self.home(s ^ 1, g)) for s, g in self.each()]


def move(array, pairs):
    return lax.ppermute(array, AXES, pairs)


def rec_body(at, ids, h_ref, w_ref, bias_ref, other_ref, z_ref):
    h = h_ref[...]
    own = ids[at["at_home"]] > 0
    count, _, width = w_ref.shape

    def block(i, carry):
        cols = pl.ds(pl.multiple_of(i * width, width), width)
        bias = jnp.where(own, bias_ref[:, cols], other_ref[:, cols])
        z_ref[:, cols] = jnp.dot(h, w_ref[i], preferred_element_type=F32) + bias
        return carry

    lax.fori_loop(0, count, block, 0)


def rec_part(at, ids, h, w_rec, bias, other):
    rows, gates = h.shape[0], bias.shape[1]
    return pl.pallas_call(
        partial(rec_body, at),
        out_shape=jax.ShapeDtypeStruct((rows, gates), F32),
        in_specs=[SMEM_SPEC] + [VMEM_SPEC] * 4,
        out_specs=VMEM_SPEC,
        name="rec_part",
        compiler_params=pltpu.CompilerParams(vmem_limit_bytes=LIMIT),
        cost_estimate=pl.CostEstimate(
            flops=2 * rows * w_rec.size, bytes_accessed=2 * w_rec.size, transcendentals=0
        ),
    )(ids, h, w_rec, bias, other)


def cell_body(at, tick, ids, edge_ref, inc_ref, z_ref, h_ref, c_ref, w_ref, h_out, c_out, gates_out):
    breadth = c_ref.shape[1]
    step = min(256, breadth)
    bottom, active = ids[at["bottom"]] > 0, ids[at["active"] + tick] > 0
    step_at = min(tick, edge_ref.shape[0] - 1)
    x = jnp.where(bottom, edge_ref[step_at, :, :breadth], inc_ref[...])
    for u in range(0, breadth, step):
        own = slice(u, u + step)
        pre = []
        for q in range(4):
            cols = slice(q * breadth + u, q * breadth + u + step)
            pre.append(z_ref[:, cols] + jnp.dot(x, w_ref[:, cols], preferred_element_type=F32))
        i = jax.nn.sigmoid(pre[0])
        f = jax.nn.sigmoid(pre[1])
        g = jnp.tanh(pre[2])
        o = jax.nn.sigmoid(pre[3])
        c_old = c_ref[:, own]
        c_new = f * c_old + i * g
        h_new = (o * jnp.tanh(c_new)).astype(BF)
        h_out[:, own] = jnp.where(active, h_new, h_ref[:, own])
        c_out[:, own] = jnp.where(active, c_new, c_old)
        for q, value in enumerate((i, f, g, o)):
            gates_out[:, q * breadth + u : q * breadth + u + step] = value


def cell_part(at, tick, ids, edge, inc, z, h, c, w_in):
    rows, breadth = c.shape
    return pl.pallas_call(
        partial(cell_body, at, tick),
        out_shape=(
            jax.ShapeDtypeStruct((rows, breadth), BF),
            jax.ShapeDtypeStruct((rows, breadth), F32),
            jax.ShapeDtypeStruct((rows, 4 * breadth), F32),
        ),
        in_specs=[SMEM_SPEC] + [VMEM_SPEC] * 6,
        out_specs=(VMEM_SPEC,) * 3,
        name="cell_part",
        compiler_params=pltpu.CompilerParams(vmem_limit_bytes=LIMIT),
        cost_estimate=pl.CostEstimate(
            flops=2 * rows * w_in.size, bytes_accessed=2 * w_in.size, transcendentals=0
        ),
    )(ids, edge, inc, z, h, c, w_in)


def nt_dot(a, b):
    return lax.dot_general(a, b, (((1,), (1,)), ((), ())), preferred_element_type=F32)


def grad_body(at, tick, sections, ids, edge_ref, inc_ref, a_ref, k_ref, gates_ref, c_ref, old_ref, *rest):
    w_ref, g_out, k_out, e_out = rest if len(rest) == 4 else (None, *rest)
    breadth = c_ref.shape[1]
    step = min(256, breadth)
    top = ids[at["top"]] > 0
    live = edge_ref[ids[at["step"] + tick], :, breadth : breadth + 1].astype(F32)
    live = live * jnp.where(ids[at["active"] + tick] > 0, 1.0, 0.0)
    cot_at = max(tick - sections + 1, 0)
    total = None
    for u in range(0, breadth, step):
        own = slice(u, u + step)
        cols = [slice(q * breadth + u, q * breadth + u + step) for q in range(4)]
        i, f, g, o = [gates_ref[:, col] for col in cols]
        above = jnp.where(top, edge_ref[cot_at, :, own], inc_ref[:, own]).astype(F32)
        dh = above + a_ref[:, own]
        squashed = jnp.tanh(c_ref[:, own])
        dc = k_ref[:, own] + dh * o * (1.0 - squashed * squashed)
        parts = (
            dc * g * i * (1.0 - i),
            dc * old_ref[:, own] * f * (1.0 - f),
            dc * i * (1.0 - g * g),
            dh * squashed * o * (1.0 - o),
        )
        k_out[:, own] = dc * f * live
        for col, part in zip(cols, parts):
            rounded = (part * live).astype(BF)
            g_out[:, col] = rounded
            if w_ref is not None:
                product = nt_dot(rounded, w_ref[:, col])
                total = product if total is None else total + product
    e_out[...] = jnp.zeros_like(e_out) if total is None else total.astype(BF)


def grad_part(at, tick, sections, ids, edge, inc, a, k, gates, c, c_old, w_in=None):
    rows, breadth = c.shape
    operands = [edge, inc, a, k, gates, c, c_old] + ([] if w_in is None else [w_in])
    return pl.pallas_call(
        partial(grad_body, at, tick, sections),
        out_shape=(
            jax.ShapeDtypeStruct((rows, 4 * breadth), BF),
            jax.ShapeDtypeStruct((rows, breadth), F32),
            jax.ShapeDtypeStruct((rows, breadth), BF),
        ),
        in_specs=[SMEM_SPEC] + [VMEM_SPEC] * len(operands),
        out_specs=(VMEM_SPEC,) * 3,
        name="grad_part",
        compiler_params=pltpu.CompilerParams(vmem_limit_bytes=LIMIT),
        cost_estimate=pl.CostEstimate(
            flops=8 * rows * breadth * breadth, bytes_accessed=8 * breadth**2, transcendentals=0
        ),
    )(ids, *operands)


def back_body(g_ref, w_ref, a_ref):
    count, _, width = w_ref.shape
    a_ref[...] = jnp.zeros_like(a_ref)

    def block(i, carry):
        cols = pl.ds(pl.multiple_of(i * width, width), width)
        a_ref[...] += nt_dot(g_ref[:, cols], w_ref[i])
        return carry

    lax.fori_loop(0, count, block, 0)


def back_part(g, w_rec):
    rows, breadth = g.shape[0], w_rec.shape[1]
    return pl.pallas_call(
        back_body,
        out_shape=jax.ShapeDtypeStruct((rows, breadth), F32),
        in_specs=[VMEM_SPEC] * 2,
        out_specs=VMEM_SPEC,
        name="back_part",
        compiler_params=pltpu.CompilerParams(vmem_limit_bytes=LIMIT),
        cost_estimate=pl.CostEstimate(
            flops=2 * rows * w_rec.size, bytes_accessed=2 * w_rec.size, transcendentals=0
        ),
    )(g, w_rec)


def collect_body(flag, places, ids, *refs):
    count = len(places)
    own, other, out, sems = refs[:count], refs[count : 2 * count], refs[-2], refs[-1]

    def copies(sources):
        return [
            pltpu.make_async_copy(
                ref, out.at[0 if places[k] is None else ids[places[k]]], sems.at[k]
            )
            for k, ref in enumerate(sources)
        ]

    @pl.when(ids[flag] > 0)
    def _():
        for copy in copies(own):
            copy.start()

    @pl.when(ids[flag] <= 0)
    def _():
        for copy in copies(other):
            copy.start()

    for copy in copies(own):
        copy.wait()


def collect(flag, places, ids, own, other, total, held=None):
    count = len(own)
    held = [] if held is None else [held]
    return pl.pallas_call(
        partial(collect_body, flag, places),
        out_shape=jax.ShapeDtypeStruct((total, *own[0].shape), own[0].dtype),
        in_specs=[SMEM_SPEC] + [ANY_SPEC] * (2 * count) + [VMEM_SPEC] * len(held),
        out_specs=VMEM_SPEC,
        scratch_shapes=[pltpu.SemaphoreType.DMA((count,))],
        input_output_aliases={2 * count + 1: 0} if held else {},
        name="collect",
        compiler_params=pltpu.CompilerParams(vmem_limit_bytes=LIMIT),
    )(ids, *own, *other, *held)


def gather_columns(roles, at, ids, block):
    if roles.groups != 8:
        whole = lax.all_gather(block, "dp", axis=1, tiled=True)
        moved = move(whole, roles.partner())
        return jnp.where(ids[at["at_home"]] > 0, whole, moved)[None]
    lines = [(a, y) for a in range(roles.sections) for y in range(2)]

    def spot(layer, m, y):
        high = (layer % 2) ^ (layer // 2 % 2)
        return roles.home(layer, 2 * (3 - m if high else m) + y)

    step1 = [(spot(a, m, y), spot(a, m - 1, y)) for a, y in lines for m in (1, 2, 3)]
    step2 = [(spot(a, m, y), spot(a, m - 1, y)) for a, y in lines for m in (1, 2)]
    step3 = [(spot(a, 1, y), spot(a, 0, y)) for a, y in lines]
    step3 += [(spot(a, 0, y), spot(a, 1, y)) for a, y in lines]
    across = [(spot(a, m, y), spot(a, m, 1 - y)) for a, y in lines for m in (0, 1)]
    beside = [(spot(a, m, y), spot(a, m, y) ^ roles.groups) for a, y in lines for m in (0, 1)]
    slots = [block, move(block, step1)]
    slots.append(move(slots[1], step2))
    nearest = ids[at["nearest"]] > 0
    slots.append(move(jnp.where(nearest, block, slots[2]), step3))
    slots += [move(slot, across) for slot in slots]
    others = [move(slot, beside) for slot in slots]
    total = None
    for chosen in ((0, 1, 2, 3, 4, 5, 6), (7,)):
        total = collect(
            at["at_home"],
            [at["slots"] + j for j in chosen],
            ids,
            [slots[j] for j in chosen],
            [others[j] for j in chosen],
            8,
            total,
        )
    return total


def gather_rows(roles, rows):
    line = [rows] + [move(rows, roles.mix(2 * k)) for k in (1, 2, 3)]
    line = jnp.stack(line)
    return line, move(line, roles.mix(1))


def split_body(at, sections, ids, *refs):
    grads, pieces = refs[: at["grads"]], refs[at["grads"] :]
    rows, width = grads[0].shape[0], pieces[0].shape[1]
    steps = pieces[0].shape[0] // rows
    for layer in range(sections):

        @pl.when(ids[at["layer"]] == layer)
        def _():
            for k, piece in enumerate(pieces):
                cols = pl.ds(pl.multiple_of(ids[at["column"] + k] * width, width), width)
                for t in range(steps):
                    piece[t * rows : (t + 1) * rows, :] = grads[layer + t][:, cols]


def scatter_columns(roles, at, ids, grads, steps):
    groups = roles.groups
    rows, gates = grads[0].shape
    pieces = pl.pallas_call(
        partial(split_body, {**at, "grads": len(grads)}, roles.sections),
        out_shape=(jax.ShapeDtypeStruct((steps * rows, gates // groups), BF),) * groups,
        in_specs=[SMEM_SPEC] + [VMEM_SPEC] * len(grads),
        out_specs=(VMEM_SPEC,) * groups,
        name="split",
        compiler_params=pltpu.CompilerParams(vmem_limit_bytes=LIMIT),
    )(ids, *grads)
    return [move(piece, roles.scatter(k)) for k, piece in enumerate(pieces)]


def pick_body(at, sections, ids, *refs):
    values, out = refs[:-1], refs[-1]
    for layer in range(sections):

        @pl.when(ids[at["layer"]] == layer)
        def _():
            for t in range(out.shape[0]):
                out[t] = values[layer + t][...]


def pick(roles, at, ids, values, steps):
    return pl.pallas_call(
        partial(pick_body, at, roles.sections),
        out_shape=jax.ShapeDtypeStruct((steps, *values[0].shape), values[0].dtype),
        in_specs=[SMEM_SPEC] + [VMEM_SPEC] * len(values),
        out_specs=VMEM_SPEC,
        name="pick",
        compiler_params=pltpu.CompilerParams(vmem_limit_bytes=LIMIT),
    )(ids, *values)


def prepare_body(at, ids, obs, cot, states, owner, burn, valid, edge, *starts):
    steps, rows, breadth = obs.shape
    last = ids[at["last"]] > 0
    for t in range(steps):
        edge[t, :, :breadth] = jnp.where(last, cot[t], obs[t])
        live = (burn[...] <= t) & (t < valid[...])
        edge[t, :, breadth:] = jnp.broadcast_to(live.astype(F32), (rows, LANES)).astype(BF)
    owned = owner[...] == ids[at["section"]]
    for k, start in enumerate(starts):
        row = states[ids[at["shift"] + k]].astype(F32)
        start[...] = jnp.where(owned, row, 0.0).astype(BF)


def prepare(at, sections, ids, obs, cot, states, owner, burn, valid):
    steps, rows, breadth = obs.shape
    column = lambda value: value.reshape(rows, 1)
    return pl.pallas_call(
        partial(prepare_body, at),
        out_shape=(
            jax.ShapeDtypeStruct((steps, rows, breadth + LANES), BF),
            *[jax.ShapeDtypeStruct((rows, 2 * breadth), BF)] * sections,
        ),
        in_specs=[SMEM_SPEC] + [VMEM_SPEC] * 6,
        out_specs=(VMEM_SPEC,) * (1 + sections),
        name="prepare",
        compiler_params=pltpu.CompilerParams(vmem_limit_bytes=LIMIT),
    )(ids, obs, cot, states, column(owner), column(burn), column(valid))


def exchange_columns(roles, grads):
    moved = move(grads, roles.to_home())
    moved = lax.all_to_all(moved, "dp", split_axis=1, concat_axis=0, tiled=True)
    return moved.reshape(roles.groups, -1, moved.shape[-1])


def turn_body(line_ref, beside_ref, out_ref):
    count, rows, _ = line_ref.shape
    for i in range(count):
        for e, ref in enumerate((line_ref, beside_ref)):
            at = (2 * i + e) * rows
            out_ref[at : at + rows, :] = ref[i]


def turn(line, beside):
    count, rows, breadth = line.shape
    return pl.pallas_call(
        turn_body,
        out_shape=jax.ShapeDtypeStruct((2 * count * rows, breadth), BF),
        in_specs=[VMEM_SPEC] * 2,
        out_specs=VMEM_SPEC,
        name="turn",
        compiler_params=pltpu.CompilerParams(vmem_limit_bytes=LIMIT),
    )(line, beside)


def outer_body(count, *refs):
    pieces, refs = refs[:count], refs[count:]
    before, alive, first, start, weight_out, bias_out, columns = refs
    rows = pieces[0].shape[0]
    for i, piece in enumerate(pieces):
        columns[i * rows : (i + 1) * rows, :] = piece[...]

    def product(a, b):
        return lax.dot_general(a, b, (((0,), (0,)), ((), ())), preferred_element_type=F32)

    weight_out[...] = product(before[...], columns[...])
    bias_out[...] = jnp.sum(columns[...].astype(F32), axis=0, keepdims=True)

    @pl.when(jnp.max(alive[...]) > 0.0)
    def _():
        weight_out[...] += product(start[...], first[...])
        bias_out[...] += jnp.sum(first[...].astype(F32), axis=0, keepdims=True)


def outer(pieces, before, alive, first, start):
    rows, width = before.shape[0], pieces[0].shape[1]
    return pl.pallas_call(
        partial(outer_body, len(pieces)),
        out_shape=(
            jax.ShapeDtypeStruct((before.shape[1], width), F32),
            jax.ShapeDtypeStruct((1, width), F32),
        ),
        in_specs=[VMEM_SPEC] * (len(pieces) + 4),
        out_specs=(VMEM_SPEC,) * 2,
        scratch_shapes=[pltpu.VMEM((rows, width), BF)],
        name="outer",
        compiler_params=pltpu.CompilerParams(vmem_limit_bytes=OUTER_LIMIT),
    )(*pieces, before, alive, first, start)


def whole_step(
    obs_features,
    w_input,
    w_recurrent,
    bias,
    stored_states,
    state_owner,
    burn_steps,
    valid_steps,
    cotangent,
):
    sections, groups = lax.axis_size("section"), lax.axis_size("dp")
    roles = Roles(sections, groups)
    steps, rows, breadth = obs_features.shape
    partner = roles.partner()
    ticks = steps + sections - 1
    table, at = roles.table(steps)
    device = lax.axis_index("section") * groups + lax.axis_index("dp")
    ids = lax.dynamic_index_in_dim(jnp.asarray(table), device, 0, keepdims=False)

    w_rec = gather_columns(roles, at, ids, w_recurrent[0])
    w_in = move(w_input[0], partner)
    w_in = collect(at["at_home"], [None], ids, [w_input[0]], [w_in], 1)[0]
    other_bias = move(bias, partner)

    edge, start, *parts = prepare(
        at,
        sections,
        ids,
        obs_features,
        cotangent,
        stored_states[0],
        state_owner,
        burn_steps,
        valid_steps,
    )
    first_live = jnp.max(edge[0, :, breadth:], axis=0, keepdims=True).astype(F32)
    first_live = jnp.broadcast_to(first_live, (8, LANES))
    edge = move(edge, roles.to_role())
    for k, part in enumerate(parts, 1):
        start = start + move(part, roles.section_shift(k))
    role_start = move(start, roles.to_role())
    bit = 1
    while bit < groups:
        first_live = jnp.maximum(first_live, move(first_live, roles.mix(bit)))
        bit *= 2
    h = role_start[:, :breadth]
    c = role_start[:, breadth:].astype(F32)

    hs, cs, gate_list = [h], [c], []
    incoming = jnp.zeros((rows, breadth), BF)
    for tick in range(ticks):
        z = rec_part(at, ids, h, w_rec, bias, other_bias)
        h, c, gates = cell_part(at, tick, ids, edge, incoming, z, h, c, w_in)
        hs.append(h)
        cs.append(c)
        gate_list.append(gates)
        if tick + 1 < ticks:
            incoming = move(h, roles.hop(1))

    hidden = pick(roles, at, ids, hs[1:], steps)
    hidden = move(hidden, roles.to_home())
    later = hidden[:-1].reshape((steps - 1) * rows, breadth)
    if groups == 8:
        later = turn(*gather_rows(roles, later))
    else:
        later = lax.all_gather(later, "dp", axis=0, tiled=True)

    def retreat(tick, incoming, a, k, gates, c, c_old, w=None):
        return grad_part(at, tick, sections, ids, edge, incoming, a, k, gates, c, c_old, w)

    grad_list = [None] * ticks
    a = jnp.zeros((rows, breadth), F32)
    k = jnp.zeros((rows, breadth), F32)
    incoming = jnp.zeros((rows, breadth), BF)
    for tick in range(ticks - 1, 0, -1):
        grads, k, lower = retreat(
            tick, incoming, a, k, gate_list[tick], cs[tick + 1], cs[tick], w_in
        )
        grad_list[tick] = grads
        incoming = move(lower, roles.hop(-1))
        a = back_part(grads, w_rec)

    if groups == 8:
        pieces = scatter_columns(roles, at, ids, grad_list[1:], steps - 1)
    else:
        grads = pick(roles, at, ids, grad_list[1:], steps - 1)
        columns = exchange_columns(roles, grads.reshape((steps - 1) * rows, 4 * breadth))
        pieces = [columns.reshape(-1, columns.shape[-1])]

    def first_step(start, incoming, a, k, gates, c, c_old, *others):
        grads, _, _ = retreat(0, incoming, a, k, gates, c, c_old)
        grads = pick(roles, at, ids, [grads, *others], 1)[0]
        columns = exchange_columns(roles, grads)
        start = lax.all_gather(start, "dp", axis=0, tiled=True)
        return columns.reshape(-1, columns.shape[-1]), start

    def no_first_step(*_):
        return (
            jnp.zeros((groups * rows, 4 * breadth // groups), BF),
            jnp.zeros((groups * rows, breadth), BF),
        )

    first, first_start = lax.cond(
        first_live[0, 0] > 0,
        first_step,
        no_first_step,
        start[:, :breadth],
        incoming,
        a,
        k,
        gate_list[0],
        cs[1],
        cs[0],
        *grad_list[1:sections],
    )
    weight_grad, bias_grad = outer(pieces, later, first_live, first, first_start)
    return (hidden[None], weight_grad[None], bias_grad)


def solution(mesh):
    in_specs = (
        P(None, "dp", None),
        P("section", None, None),
        P("section", None, "dp"),
        P("section", None),
        P("section", None, "dp", None),
        P("dp"),
        P("dp"),
        P("dp"),
        P(None, "dp", None),
    )
    out_specs = (P("section", None, "dp", None), P("section", None, "dp"), P("section", "dp"))
    return jax.shard_map(
        whole_step, mesh=mesh, in_specs=in_specs, out_specs=out_specs, check_vma=False
    )
```
